32 devices in a mesh: gx: 32 (over z, y, x, core).
Axes of the slice: x: 2, y: 2, z: 4, core: 2. Of those that a mesh axis runs over, the one named last changes fastest.
Arguments:
- fine: bfloat16 [64, 8192, 128], P(None, 'gx'), may hold values from -6 to 6
- pattern: int32 [8, 8192], P(None, 'gx'), may hold values from 0 to 3
- stencil: bfloat16 [3, 128, 128], replicated, may hold values from -0.3125 to 0.3125
- restrict: bfloat16 [8, 4, 128, 128], replicated, may hold values from -0.5 to 0.5
- coarse_inv: bfloat16 [8, 128, 128], replicated, may hold values from -0.5 to 0.5
Outputs:
- smoothed: float32 [64, 8192, 128], P(None, 'gx')
The draws below stay inside these ranges and needn't reach their ends.
All inputs are finite; a program needn't handle non-finite values.
Results may differ from the reference program's by a relative error of at most 0.0046.
Values may be sent and summed in bfloat16 or wider, within the bound.
A program may use at most 128 MiB of HBM per device.

```python
import jax
import jax.numpy as jnp
from jax import lax

WIDTH = 128
KINDS = 4
LEVELS = 8
BLK_DEV = 256
NVEC = 64
NB = 8192


def touch_ends(values, rng, least, high):
    place = [jax.random.randint(jax.random.fold_in(rng, axis), (), 0, length) for axis, length in enumerate(values.shape)]
    widest = values.shape.index(max(values.shape))
    next_to = place[:widest] + [(place[widest] + 1) % values.shape[widest]] + place[widest + 1:]
    return values.at[tuple(place)].set(least).at[tuple(next_to)].set(high)


def block_levels(key, shape, pieces, low, top_value):
    def one(axis_at, parts):
        steps = jax.random.uniform(jax.random.fold_in(jax.random.fold_in(key, 6), axis_at), (parts,), jnp.float32, low / len(pieces), top_value / len(pieces))
        return jnp.repeat(jnp.exp(steps), shape[axis_at] // parts).reshape((-1,) + (1,) * (len(shape) - axis_at - 1))

    factor_of = one(*pieces[0])
    for cut in pieces[1:]:
        factor_of = factor_of * one(*cut)
    return factor_of


def gaussian(rng, dims, scale, reach, cuts=(), held_as=jnp.bfloat16):
    values = jax.random.normal(rng, dims, jnp.float32) * scale
    if len(cuts) > 0:
        values = block_levels(rng, dims, cuts, -0.22, 0.18) * values
    return jnp.clip(values, min=-reach, max=reach).astype(held_as)


def setup_inputs(seed: int = 0) -> dict:
    key_list = jax.random.split(jax.random.key(seed), 6)
    fine = gaussian(key_list[0], (NVEC, NB, WIDTH), 1.0, 6.0, ((1, 32),))
    pattern = touch_ends(jax.random.randint(key_list[1], (LEVELS, NB), 0, KINDS), jax.random.fold_in(key_list[1], 1), 0, KINDS - 1).astype(jnp.int32)
    stencil = gaussian(key_list[2], (3, WIDTH, WIDTH), (3 * WIDTH) ** -0.5, 0.3125)
    restrict = gaussian(key_list[3], (LEVELS, KINDS, WIDTH, WIDTH), WIDTH ** -0.5, 0.5)
    coarse_inv = gaussian(key_list[4], (LEVELS, WIDTH, WIDTH), WIDTH ** -0.5, 0.5)
    return {"fine": fine, "pattern": pattern, "stencil": stencil, "restrict": restrict, "coarse_inv": coarse_inv}


EXACT = lax.Precision.HIGHEST


def one_vector(fine_vec, pattern, stencil, restrict, coarse_inv):
    all_blocks = fine_vec.shape[0]
    width = fine_vec.shape[1]
    earlier = jnp.roll(fine_vec, 1, axis=0)
    later = jnp.roll(fine_vec, -1, axis=0)
    result = jnp.dot(earlier, stencil[0], preferred_element_type=jnp.float32)
    result = result + jnp.dot(fine_vec, stencil[1], preferred_element_type=jnp.float32)
    result = result + jnp.dot(later, stencil[2], preferred_element_type=jnp.float32)
    widened = fine_vec.astype(jnp.float32)
    kinds_row = jnp.arange(KINDS, dtype=jnp.int32)
    for level_num in range(LEVELS):
        coarse_num = max(all_blocks // 4 ** (level_num + 1), 1)
        span_blocks = all_blocks // coarse_num
        run_len = min(span_blocks, BLK_DEV)
        run_num = all_blocks // run_len
        selector = pattern[level_num][:, None] == kinds_row[None, :]
        onehot = selector.astype(jnp.float32).reshape(run_num, run_len, KINDS)
        tiles = restrict[level_num].astype(jnp.float32)
        grouped = jnp.einsum("nsc,nsk->nkc", widened.reshape(run_num, run_len, width), onehot, precision=EXACT)
        grouped = grouped.astype(jnp.bfloat16).astype(jnp.float32)
        per_run = jnp.einsum("nkc,kcd->nd", grouped, tiles, precision=EXACT)
        coarse = jnp.sum(per_run.reshape(coarse_num, span_blocks // run_len, width), axis=1) * (span_blocks ** -0.5)
        rounded = coarse.astype(jnp.bfloat16)
        solved = jnp.dot(rounded, coarse_inv[level_num], preferred_element_type=jnp.float32).astype(jnp.bfloat16)
        lifted = jnp.einsum("jd,kcd->jkc", solved.astype(jnp.float32), tiles, precision=EXACT)
        kind_map = pattern[level_num].reshape(coarse_num, span_blocks)
        for kind_num in range(KINDS):
            chosen = (kind_map == kind_num)[:, :, None]
            part_add = jnp.where(chosen, lifted[:, kind_num][:, None, :], jnp.float32(0.0))
            result = result + part_add.reshape(all_blocks, width)
    return result


def reference(fine, pattern, stencil, restrict, coarse_inv):
    return lax.map(lambda fine_vec: one_vector(fine_vec, pattern, stencil, restrict, coarse_inv), fine)
```

```python
import functools

import jax
import jax.numpy as jnp
from jax import lax
from jax.experimental import pallas as pl
from jax.experimental.pallas import tpu as pltpu
from jax.sharding import PartitionSpec as P

MESH = pl.DeviceIdType.MESH
F32 = jnp.float32
BF16 = jnp.bfloat16
TILE = 16
VMEM_LIMIT = 40 * 2**20


def round_up(value, unit):
    return -(-value // unit) * unit


class Plan:
    def __init__(self, devices, vectors, blocks, width, levels, kinds):
        self.devices, self.vectors, self.blocks = devices, vectors, blocks
        self.width, self.levels, self.kinds = width, levels, kinds
        all_blocks = devices * blocks
        self.spans, self.local_spans, self.counts, self.groups = [], [], [], []
        for level in range(levels):
            span = all_blocks // max(all_blocks // 4 ** (level + 1), 1)
            local = min(span, blocks)
            self.spans.append(span)
            self.local_spans.append(local)
            self.counts.append(blocks // local)
            self.groups.append(span // local)
        self.narrow = [l for l in range(levels) if self.counts[l] > 1]
        self.wide = [l for l in range(levels) if self.counts[l] == 1]
        self.crossing = [l for l in range(levels) if self.groups[l] > 1]
        self.padded = {l: round_up(self.counts[l], TILE) for l in self.narrow}
        self.offsets, at = {}, 0
        for l in self.narrow:
            self.offsets[l] = at
            at += kinds * self.padded[l]
        self.narrow_rows = at
        self.wide_used = len(self.wide) * kinds + 2
        self.wide_rows = round_up(self.wide_used, TILE)


def wide_rows_onehot(plan, pattern, rows_axis):
    shape = (plan.wide_rows, plan.blocks) if rows_axis == 0 else (plan.blocks, plan.wide_rows)
    row = lax.broadcasted_iota(jnp.int32, shape, rows_axis)
    block = lax.broadcasted_iota(jnp.int32, shape, 1 - rows_axis)
    base = len(plan.wide) * plan.kinds
    hit = ((row == base) & (block == 0)) | ((row == base + 1) & (block == plan.blocks - 1))
    for position, level in enumerate(plan.wide):
        kinds = pattern[level : level + 1, :] if rows_axis == 0 else pattern[:, level : level + 1]
        first = position * plan.kinds
        inside = (row >= first) & (row < first + plan.kinds)
        hit = hit | (inside & (row - first == kinds))
    return hit.astype(F32).astype(BF16)


def narrow_onehot(plan, pattern, level, rows_axis):
    padded = plan.padded[level]
    rows = plan.kinds * padded
    shape = (rows, plan.blocks) if rows_axis == 0 else (plan.blocks, rows)
    row = lax.broadcasted_iota(jnp.int32, shape, rows_axis)
    block = lax.broadcasted_iota(jnp.int32, shape, 1 - rows_axis)
    kinds = pattern[level : level + 1, :] if rows_axis == 0 else pattern[:, level : level + 1]
    target = kinds * padded + block // plan.local_spans[level]
    return (row == target).astype(F32).astype(BF16)


def pair_of(ref, first):
    return jnp.concatenate([ref[first], ref[first + 1]], axis=1)


def wide_kernel(plan, chunk, pattern_ref, fine_ref, restrict_ref, coarse_ref, halo_ref, onehot, grouped, rows):
    step = pl.program_id(0)
    width = plan.width

    @pl.when(step == 0)
    def _():
        onehot[...] = wide_rows_onehot(plan, pattern_ref[...], 0)

    for first in range(0, chunk, 2):
        both = jnp.dot(onehot[...], pair_of(fine_ref, first), preferred_element_type=F32)
        grouped[first] = both[:, :width]
        grouped[first + 1] = both[:, width:]
    here = pl.ds(pl.multiple_of(step * chunk, chunk), chunk)
    for row in range(plan.wide_used):
        rows[row, here, :] = grouped[:, row, :].astype(BF16)

    @pl.when(step == pl.num_programs(0) - 1)
    def _():
        for position, level in enumerate(plan.wide):
            first = position * plan.kinds
            joined = jnp.concatenate([rows[first + kind] for kind in range(plan.kinds)], axis=1)
            coarse = jnp.dot(joined, restrict_ref[level], preferred_element_type=F32)
            coarse_ref[position] = (coarse * plan.spans[level] ** (-0.5)).astype(BF16)
        base = len(plan.wide) * plan.kinds
        halo_ref[0] = rows[base]
        halo_ref[1] = rows[base + 1]


def exchange_kernel(plan, coarse_ref, halo_ref, sums_ref, beside_ref, *scratch):
    (from_group, to_column, from_column, to_group, back, group_send, group_recv,
     column_send, column_recv, back_send, back_recv, halo_send, halo_recv) = scratch
    devices = plan.devices
    near = plan.groups[plan.crossing[0]]
    far = devices // near
    local = len(plan.wide) - len(plan.crossing)
    crossing = len(plan.crossing)
    part = plan.vectors // near
    me = lax.axis_index("gx")
    mine = lax.rem(me, near)
    place = me // near

    def group_peer(apart):
        return place * near + lax.rem(mine + apart, near)

    def column_peer(apart):
        return lax.rem(place + apart, far) * near + mine

    nexts = lax.rem(me + 1, devices)
    previous = lax.rem(me + devices - 1, devices)
    barrier = pltpu.get_barrier_semaphore()
    peers = [group_peer(a) for a in range(1, near)] + [column_peer(a) for a in range(1, far)] + [nexts, previous]
    for peer in peers:
        pl.semaphore_signal(barrier, inc=1, device_id=(peer,), device_id_type=MESH)
    pl.semaphore_wait(barrier, len(peers))

    def part_of(index):
        return pl.ds(pl.multiple_of(index * part, part), part)

    copies = []
    for apart in range(1, near):
        theirs = lax.rem(mine + apart, near)
        copies.append(pltpu.make_async_remote_copy(
            src_ref=coarse_ref.at[pl.ds(local, crossing), part_of(theirs), :],
            dst_ref=from_group.at[apart],
            send_sem=group_send.at[apart], recv_sem=group_recv.at[apart],
            device_id=(group_peer(apart),), device_id_type=MESH))
    halo_copies = []
    for side, peer in ((0, previous), (1, nexts)):
        halo_copies.append(pltpu.make_async_remote_copy(
            src_ref=halo_ref.at[side], dst_ref=beside_ref.at[1 - side],
            send_sem=halo_send.at[side], recv_sem=halo_recv.at[1 - side],
            device_id=(peer,), device_id_type=MESH))
    for copy in copies + halo_copies:
        copy.start()
    total = coarse_ref[pl.ds(local, crossing), part_of(mine), :].astype(F32)
    for apart, copy in enumerate(copies, 1):
        copy.wait_recv()
        total = total + from_group[apart].astype(F32)
    to_column[...] = total.astype(BF16)

    column_copies = []
    for apart in range(1, far):
        column_copies.append(pltpu.make_async_remote_copy(
            src_ref=to_column.at[pl.ds(1, crossing - 1)], dst_ref=from_column.at[apart],
            send_sem=column_send.at[apart], recv_sem=column_recv.at[apart],
            device_id=(column_peer(apart),), device_id_type=MESH))
    for copy in column_copies:
        copy.start()
    sums = [total[index] for index in range(crossing)]
    for apart, copy in enumerate(column_copies, 1):
        copy.wait_recv()
        source = lax.rem(place + far - apart, far)
        for index in range(1, crossing):
            reach = plan.groups[plan.crossing[index]] // near
            keep = (source // reach == place // reach).astype(F32)
            sums[index] = sums[index] + keep * from_column[apart, index - 1].astype(F32)
    for index in range(crossing):
        to_group[index] = sums[index].astype(BF16)

    back_copies = []
    for apart in range(1, near):
        back_copies.append(pltpu.make_async_remote_copy(
            src_ref=to_group, dst_ref=back.at[apart],
            send_sem=back_send.at[apart], recv_sem=back_recv.at[apart],
            device_id=(group_peer(apart),), device_id_type=MESH))
    for copy in back_copies:
        copy.start()
    for index in range(local):
        sums_ref[index] = coarse_ref[index]
    sums_ref[pl.ds(local, crossing), part_of(mine), :] = to_group[...]
    for apart, copy in enumerate(back_copies, 1):
        copy.wait_recv()
        source = lax.rem(mine + near - apart, near)
        sums_ref[pl.ds(local, crossing), part_of(source), :] = back[apart]
    for copy in halo_copies:
        copy.wait_recv()
    for copy in copies + halo_copies + column_copies + back_copies:
        copy.wait_send()


def narrow_kernel(plan, chunk, pattern_ref, fine_ref, restrict_ref, inverse_ref, lifted_ref, onehot, grouped):
    width = plan.width

    @pl.when(pl.program_id(0) == 0)
    def _():
        for level in plan.narrow:
            rows = pl.ds(plan.offsets[level], plan.kinds * plan.padded[level])
            onehot[rows, :] = narrow_onehot(plan, pattern_ref[...], level, 0)

    for first in range(0, chunk, 2):
        both = jnp.dot(onehot[...], pair_of(fine_ref, first), preferred_element_type=F32).astype(BF16)
        grouped[first] = both[:, :width]
        grouped[first + 1] = both[:, width:]
    for level in plan.narrow:
        padded = plan.padded[level]
        slices = [pl.ds(plan.offsets[level] + kind * padded, padded) for kind in range(plan.kinds)]
        joined = jnp.concatenate(
            [grouped[:, rows, :].reshape(chunk * padded, width) for rows in slices], axis=1)
        coarse = jnp.dot(joined, restrict_ref[level], preferred_element_type=F32)
        rounded = (coarse * plan.spans[level] ** (-0.5)).astype(BF16)
        solved = jnp.dot(rounded, inverse_ref[level], preferred_element_type=F32).astype(BF16)
        lifted = lax.dot_general(
            solved, restrict_ref[level], (((1,), (1,)), ((), ())), preferred_element_type=F32).astype(BF16)
        for kind, rows in enumerate(slices):
            lifted_ref[:, rows, :] = lifted[:, kind * width : (kind + 1) * width].reshape(chunk, padded, width)


def final_kernel(plan, chunk, pattern_ref, sums_ref, beside_ref, stencil_ref, restrict_ref, inverse_ref,
                 fine_ref, lifted_ref, out_ref, spread, wide_lifted, before, after):
    step = pl.program_id(0)
    width, blocks, kinds = plan.width, plan.blocks, plan.kinds

    @pl.when(step == 0)
    def _():
        turned = pattern_ref[...].T
        for level in plan.narrow:
            columns = pl.ds(plan.offsets[level], kinds * plan.padded[level])
            spread[:, columns] = narrow_onehot(plan, turned, level, 1)
        spread[:, pl.ds(plan.narrow_rows, plan.wide_rows)] = wide_rows_onehot(plan, turned, 1)
        for position, level in enumerate(plan.wide):
            solved = jnp.dot(sums_ref[position], inverse_ref[level], preferred_element_type=F32).astype(BF16)
            lifted = lax.dot_general(
                solved, restrict_ref[level], (((1,), (1,)), ((), ())), preferred_element_type=F32)
            for kind in range(kinds):
                wide_lifted[:, position * kinds + kind, :] = lifted[:, kind * width : (kind + 1) * width]
        base = len(plan.wide) * kinds
        wide_lifted[:, base, :] = jnp.dot(beside_ref[0], stencil_ref[0], preferred_element_type=F32)
        wide_lifted[:, base + 1, :] = jnp.dot(beside_ref[1], stencil_ref[2], preferred_element_type=F32)
        for row in range(plan.wide_used, plan.wide_rows):
            wide_lifted[:, row, :] = jnp.zeros((plan.vectors, width), F32)
        for slot in range(2):
            before[slot, pl.ds(0, 8), :] = jnp.zeros((8, width), F32)
            after[slot, pl.ds(blocks, 8), :] = jnp.zeros((8, width), F32)

    stencils = jnp.concatenate([stencil_ref[0], stencil_ref[1], stencil_ref[2]], axis=1)
    for first in range(0, chunk, 2):
        tables = []
        for slot in range(2):
            vector = step * chunk + first + slot
            tables.append(jnp.concatenate([lifted_ref[first + slot], wide_lifted[vector].astype(BF16)], axis=0))
        both = jnp.dot(spread[...], jnp.concatenate(tables, axis=1), preferred_element_type=F32)
        for slot in range(2):
            three = jnp.dot(fine_ref[first + slot], stencils, preferred_element_type=F32)
            before[slot, pl.ds(8, blocks), :] = three[:, :width]
            after[slot, pl.ds(0, blocks), :] = three[:, 2 * width :]
            result = both[:, slot * width : (slot + 1) * width] + three[:, width : 2 * width]
            result = result + before[slot, pl.ds(7, blocks), :]
            out_ref[first + slot] = result + after[slot, pl.ds(1, blocks), :]


def whole(ndim_shape):
    return pl.BlockSpec(ndim_shape, lambda *_: (0,) * len(ndim_shape))


def shards(fine, pattern, stencil, restrict, coarse_inv):
    devices = lax.axis_size("gx")
    vectors, blocks, width = fine.shape
    levels, kinds = restrict.shape[:2]
    plan = Plan(devices, vectors, blocks, width, levels, kinds)
    stacked = restrict.reshape(levels, kinds * width, width)
    wide_count = len(plan.wide)
    params = pltpu.CompilerParams(dimension_semantics=("arbitrary",), vmem_limit_bytes=VMEM_LIMIT)

    chunk = 16
    fine_spec = pl.BlockSpec((chunk, blocks, width), lambda i: (i, 0, 0))
    coarse, halo = pl.pallas_call(
        functools.partial(wide_kernel, plan, chunk),
        grid=(vectors // chunk,),
        out_shape=(jax.ShapeDtypeStruct((wide_count, vectors, width), BF16),
                   jax.ShapeDtypeStruct((2, vectors, width), BF16)),
        in_specs=[whole(pattern.shape), fine_spec, whole(stacked.shape)],
        out_specs=(whole((wide_count, vectors, width)), whole((2, vectors, width))),
        scratch_shapes=[
            pltpu.VMEM((plan.wide_rows, blocks), BF16),
            pltpu.VMEM((chunk, plan.wide_rows, width), F32),
            pltpu.VMEM((plan.wide_used, vectors, width), BF16),
        ],
        compiler_params=params,
        name="wide",
    )(pattern, fine, stacked)

    near = plan.groups[plan.crossing[0]]
    far = devices // near
    crossing = len(plan.crossing)
    part = vectors // near
    vmem = pl.BlockSpec(memory_space=pltpu.VMEM)
    dma = pltpu.SemaphoreType.DMA
    sums, beside = pl.pallas_call(
        functools.partial(exchange_kernel, plan),
        out_shape=(jax.ShapeDtypeStruct(coarse.shape, BF16), jax.ShapeDtypeStruct(halo.shape, BF16)),
        in_specs=[vmem, vmem],
        out_specs=(vmem, vmem),
        scratch_shapes=[
            pltpu.VMEM((near, crossing, part, width), BF16),
            pltpu.VMEM((crossing, part, width), BF16),
            pltpu.VMEM((far, crossing - 1, part, width), BF16),
            pltpu.VMEM((crossing, part, width), BF16),
            pltpu.VMEM((near, crossing, part, width), BF16),
            dma((near,)), dma((near,)), dma((far,)), dma((far,)), dma((near,)), dma((near,)), dma((2,)), dma((2,)),
        ],
        compiler_params=pltpu.CompilerParams(collective_id=0, has_side_effects=True),
        name="exchange",
    )(coarse, halo)

    lifted = pl.pallas_call(
        functools.partial(narrow_kernel, plan, chunk),
        grid=(vectors // chunk,),
        out_shape=jax.ShapeDtypeStruct((vectors, plan.narrow_rows, width), BF16),
        in_specs=[whole(pattern.shape), fine_spec, whole(stacked.shape), whole(coarse_inv.shape)],
        out_specs=pl.BlockSpec((chunk, plan.narrow_rows, width), lambda i: (i, 0, 0)),
        scratch_shapes=[
            pltpu.VMEM((plan.narrow_rows, blocks), BF16),
            pltpu.VMEM((chunk, plan.narrow_rows, width), BF16),
        ],
        compiler_params=params,
        name="narrow",
    )(pattern, fine, stacked, coarse_inv)

    last = 8
    return pl.pallas_call(
        functools.partial(final_kernel, plan, last),
        grid=(vectors // last,),
        out_shape=jax.ShapeDtypeStruct(fine.shape, F32),
        in_specs=[
            whole(pattern.shape), whole(sums.shape), whole(beside.shape), whole(stencil.shape),
            whole(stacked.shape), whole(coarse_inv.shape),
            pl.BlockSpec((last, blocks, width), lambda i: (i, 0, 0)),
            pl.BlockSpec((last, plan.narrow_rows, width), lambda i: (i, 0, 0)),
        ],
        out_specs=pl.BlockSpec((last, blocks, width), lambda i: (i, 0, 0)),
        scratch_shapes=[
            pltpu.VMEM((blocks, plan.narrow_rows + plan.wide_rows), BF16),
            pltpu.VMEM((vectors, plan.wide_rows, width), F32),
            pltpu.VMEM((2, blocks + 8, width), F32),
            pltpu.VMEM((2, blocks + 8, width), F32),
        ],
        compiler_params=params,
        name="final",
    )(pattern, sums, beside, stencil, stacked, coarse_inv, fine, lifted)


def solution(mesh):
    in_specs = (P(None, "gx", None), P(None, "gx"), P(), P(), P())
    out_specs = P(None, "gx", None)
    return jax.shard_map(shards, mesh=mesh, in_specs=in_specs, out_specs=out_specs, check_vma=False)
```

```python
import functools

import jax
import jax.numpy as jnp
from jax import lax
from jax.experimental import pallas as pl
from jax.experimental.pallas import tpu as pltpu
from jax.sharding import PartitionSpec as P

MESH = pl.DeviceIdType.MESH
F32 = jnp.float32
BF16 = jnp.bfloat16
TILE = 16
VMEM_LIMIT = 63 * 2**20


def round_up(value, unit):
    return -(-value // unit) * unit


class Plan:
    def __init__(self, devices, vectors, blocks, width, levels, kinds):
        self.devices, self.vectors, self.blocks = devices, vectors, blocks
        self.width, self.levels, self.kinds = width, levels, kinds
        all_blocks = devices * blocks
        self.spans, self.local_spans, self.counts, self.groups = [], [], [], []
        for level in range(levels):
            span = all_blocks // max(all_blocks // 4 ** (level + 1), 1)
            local = min(span, blocks)
            self.spans.append(span)
            self.local_spans.append(local)
            self.counts.append(blocks // local)
            self.groups.append(span // local)
        self.narrow = [l for l in range(levels) if self.counts[l] > 1]
        self.wide = [l for l in range(levels) if self.counts[l] == 1]
        self.crossing = [l for l in range(levels) if self.groups[l] > 1]
        self.padded = {l: round_up(self.counts[l], TILE) for l in self.narrow}
        self.offsets, at = {}, 0
        for l in self.narrow:
            self.offsets[l] = at
            at += kinds * self.padded[l]
        self.narrow_rows = at
        self.wide_used = len(self.wide) * kinds + 2
        self.wide_rows = round_up(self.wide_used, TILE)


def wide_rows_onehot(plan, pattern, rows_axis):
    shape = (plan.wide_rows, plan.blocks) if rows_axis == 0 else (plan.blocks, plan.wide_rows)
    row = lax.broadcasted_iota(jnp.int32, shape, rows_axis)
    block = lax.broadcasted_iota(jnp.int32, shape, 1 - rows_axis)
    base = len(plan.wide) * plan.kinds
    hit = ((row == base) & (block == 0)) | ((row == base + 1) & (block == plan.blocks - 1))
    for position, level in enumerate(plan.wide):
        kinds = pattern[level : level + 1, :] if rows_axis == 0 else pattern[:, level : level + 1]
        first = position * plan.kinds
        inside = (row >= first) & (row < first + plan.kinds)
        hit = hit | (inside & (row - first == kinds))
    return hit.astype(F32).astype(BF16)


def narrow_onehot(plan, pattern, level, rows_axis):
    padded = plan.padded[level]
    rows = plan.kinds * padded
    shape = (rows, plan.blocks) if rows_axis == 0 else (plan.blocks, rows)
    row = lax.broadcasted_iota(jnp.int32, shape, rows_axis)
    block = lax.broadcasted_iota(jnp.int32, shape, 1 - rows_axis)
    kinds = pattern[level : level + 1, :] if rows_axis == 0 else pattern[:, level : level + 1]
    target = kinds * padded + block // plan.local_spans[level]
    return (row == target).astype(F32).astype(BF16)


def exchange_kernel(plan, chunk, pattern_ref, fine_hbm, restrict_hbm, inverse_hbm, lifted_hbm, wide_hbm, beside_ref,
                    fine_ref, restrict_ref, inverse_ref, lifted_ref, wide_ref, wide_f32, wide_onehot, onehot, few,
                    grouped, rows, coarse_ref, halo_ref,
                    from_group, to_column, from_column, to_group, back,
                    fine_sem, weight_sem, lifted_sem, wide_sem, group_send, group_recv,
                    column_send, column_recv, back_send, back_recv, halo_send, halo_recv):
    width, kinds = plan.width, plan.kinds
    steps = plan.vectors // chunk
    devices = plan.devices
    near = plan.groups[plan.crossing[0]]
    far = devices // near
    local = len(plan.wide) - len(plan.crossing)
    crossing = len(plan.crossing)
    part = plan.vectors // near
    me = lax.axis_index("gx")
    mine = lax.rem(me, near)
    place = me // near

    def chunk_of(step):
        return pl.ds(pl.multiple_of(step * chunk, chunk), chunk)

    def fine_copy(step):
        return pltpu.make_async_copy(fine_hbm.at[chunk_of(step)], fine_ref.at[chunk_of(step)], fine_sem.at[step])

    def lifted_copy(step):
        return pltpu.make_async_copy(lifted_ref.at[chunk_of(step)], lifted_hbm.at[chunk_of(step)], lifted_sem.at[step])

    weight_copies = [
        pltpu.make_async_copy(restrict_hbm, restrict_ref, weight_sem.at[0]),
        pltpu.make_async_copy(inverse_hbm, inverse_ref, weight_sem.at[1]),
    ]
    for step in range(steps):
        fine_copy(step).start()
    for copy in weight_copies:
        copy.start()

    def group_peer(apart):
        return place * near + lax.rem(mine + apart, near)

    def column_peer(apart):
        return lax.rem(place + apart, far) * near + mine

    nexts = lax.rem(me + 1, devices)
    previous = lax.rem(me + devices - 1, devices)
    barrier = pltpu.get_barrier_semaphore()
    peers = [group_peer(a) for a in range(1, near)] + [column_peer(a) for a in range(1, far)] + [nexts, previous]
    for peer in peers:
        pl.semaphore_signal(barrier, inc=1, device_id=(peer,), device_id_type=MESH)

    wide_onehot[...] = wide_rows_onehot(plan, pattern_ref[...], 0)

    def gather_wide(step, _):
        fine_copy(step).wait()
        here = chunk_of(step)
        for first in range(0, chunk, 2):
            at = step * chunk + first
            both = jnp.concatenate([fine_ref[at], fine_ref[at + 1]], axis=1)
            both = jnp.dot(wide_onehot[...], both, preferred_element_type=F32)
            few[first] = both[:, :width]
            few[first + 1] = both[:, width:]
        for row in range(plan.wide_used):
            rows[row, here, :] = few[:, row, :].astype(BF16)
        return 0

    lax.fori_loop(0, steps, gather_wide, 0)
    for copy in weight_copies:
        copy.wait()
    for position, level in enumerate(plan.wide):
        first = position * kinds
        joined = jnp.concatenate([rows[first + kind] for kind in range(kinds)], axis=1)
        coarse = jnp.dot(joined, restrict_ref[level], preferred_element_type=F32)
        coarse_ref[position] = (coarse * plan.spans[level] ** (-0.5)).astype(BF16)
    base = len(plan.wide) * kinds
    halo_ref[0] = rows[base]
    halo_ref[1] = rows[base + 1]

    pl.semaphore_wait(barrier, len(peers))

    def part_of(index):
        return pl.ds(pl.multiple_of(index * part, part), part)

    copies = []
    for apart in range(1, near):
        theirs = lax.rem(mine + apart, near)
        copies.append(pltpu.make_async_remote_copy(
            src_ref=coarse_ref.at[pl.ds(local, crossing), part_of(theirs), :],
            dst_ref=from_group.at[apart],
            send_sem=group_send.at[apart], recv_sem=group_recv.at[apart],
            device_id=(group_peer(apart),), device_id_type=MESH))
    halo_copies = []
    for side, peer in ((0, previous), (1, nexts)):
        halo_copies.append(pltpu.make_async_remote_copy(
            src_ref=halo_ref.at[side], dst_ref=beside_ref.at[1 - side],
            send_sem=halo_send.at[side], recv_sem=halo_recv.at[1 - side],
            device_id=(peer,), device_id_type=MESH))
    for copy in copies + halo_copies:
        copy.start()

    for level in plan.narrow:
        onehot[pl.ds(plan.offsets[level], kinds * plan.padded[level]), :] = narrow_onehot(
            plan, pattern_ref[...], level, 0)

    def narrow(step, _):
        here = chunk_of(step)
        for first in range(0, chunk, 2):
            at = step * chunk + first
            both = jnp.concatenate([fine_ref[at], fine_ref[at + 1]], axis=1)
            both = jnp.dot(onehot[...], both, preferred_element_type=F32).astype(BF16)
            grouped[first] = both[:, :width]
            grouped[first + 1] = both[:, width:]
        for level in plan.narrow:
            padded = plan.padded[level]
            slices = [pl.ds(plan.offsets[level] + kind * padded, padded) for kind in range(kinds)]
            joined = jnp.concatenate(
                [grouped[:, tile, :].reshape(chunk * padded, width) for tile in slices], axis=1)
            coarse = jnp.dot(joined, restrict_ref[level], preferred_element_type=F32)
            rounded = (coarse * plan.spans[level] ** (-0.5)).astype(BF16)
            solved = jnp.dot(rounded, inverse_ref[level], preferred_element_type=F32).astype(BF16)
            lifted = lax.dot_general(
                solved, restrict_ref[level], (((1,), (1,)), ((), ())), preferred_element_type=F32).astype(BF16)
            for kind, tile in enumerate(slices):
                lifted_ref[here, tile, :] = lifted[:, kind * width : (kind + 1) * width].reshape(chunk, padded, width)
        lifted_copy(step).start()
        return 0

    def lift_wide(position, rounded):
        level = plan.wide[position]
        solved = jnp.dot(rounded, inverse_ref[level], preferred_element_type=F32).astype(BF16)
        lifted = lax.dot_general(
            solved, restrict_ref[level], (((1,), (1,)), ((), ())), preferred_element_type=F32)
        for kind in range(kinds):
            wide_f32[:, position * kinds + kind, :] = lifted[:, kind * width : (kind + 1) * width]

    first_stop = steps // 4
    second_stop = steps - max(steps // 4, 1)
    lax.fori_loop(0, first_stop, narrow, 0)

    total = coarse_ref[pl.ds(local, crossing), part_of(mine), :].astype(F32)
    for apart, copy in enumerate(copies, 1):
        copy.wait_recv()
        total = total + from_group[apart].astype(F32)
    to_column[...] = total.astype(BF16)

    column_copies = []
    for apart in range(1, far):
        column_copies.append(pltpu.make_async_remote_copy(
            src_ref=to_column.at[pl.ds(1, crossing - 1)], dst_ref=from_column.at[apart],
            send_sem=column_send.at[apart], recv_sem=column_recv.at[apart],
            device_id=(column_peer(apart),), device_id_type=MESH))
    for copy in column_copies:
        copy.start()

    for row in range(plan.wide_used, plan.wide_rows):
        wide_f32[:, row, :] = jnp.zeros((plan.vectors, width), F32)
    for position in range(local):
        lift_wide(position, coarse_ref[position])
    lax.fori_loop(first_stop, second_stop, narrow, 0)

    to_group[0] = to_column[0]
    sums = [to_column[index].astype(F32) for index in range(crossing)]
    for apart, copy in enumerate(column_copies, 1):
        copy.wait_recv()
        source = lax.rem(place + far - apart, far)
        for index in range(1, crossing):
            reach = plan.groups[plan.crossing[index]] // near
            keep = (source // reach == place // reach).astype(F32)
            sums[index] = sums[index] + keep * from_column[apart, index - 1].astype(F32)
    for index in range(1, crossing):
        to_group[index] = sums[index].astype(BF16)

    back_copies = []
    for apart in range(1, near):
        back_copies.append(pltpu.make_async_remote_copy(
            src_ref=to_group, dst_ref=back.at[apart],
            send_sem=back_send.at[apart], recv_sem=back_recv.at[apart],
            device_id=(group_peer(apart),), device_id_type=MESH))
    for copy in back_copies:
        copy.start()

    lax.fori_loop(second_stop, steps, narrow, 0)
    for copy in halo_copies:
        copy.wait_recv()
    for copy in copies:
        copy.wait_send()
    coarse_ref[pl.ds(local, crossing), part_of(mine), :] = to_group[...]
    for apart, copy in enumerate(back_copies, 1):
        copy.wait_recv()
        source = lax.rem(mine + near - apart, near)
        coarse_ref[pl.ds(local, crossing), part_of(source), :] = back[apart]
    for position in range(local, len(plan.wide)):
        lift_wide(position, coarse_ref[position])
    wide_ref[...] = wide_f32[...].astype(BF16)
    wide_copy = pltpu.make_async_copy(wide_ref, wide_hbm, wide_sem)
    wide_copy.start()
    for step in range(steps):
        lifted_copy(step).wait()
    for copy in halo_copies + column_copies + back_copies:
        copy.wait_send()
    wide_copy.wait()


def final_kernel(plan, chunk, pattern_ref, beside_ref, stencil_ref,
                 fine_ref, lifted_ref, wide_ref, out_ref, spread, halo, before, after):
    step = pl.program_id(0)
    width, blocks = plan.width, plan.blocks

    @pl.when(step == 0)
    def _():
        turned = pattern_ref[...].T
        for level in plan.narrow:
            columns = pl.ds(plan.offsets[level], plan.kinds * plan.padded[level])
            spread[:, columns] = narrow_onehot(plan, turned, level, 1)
        spread[:, pl.ds(plan.narrow_rows, plan.wide_rows)] = wide_rows_onehot(plan, turned, 1)
        halo[0] = jnp.dot(beside_ref[0], stencil_ref[0], preferred_element_type=F32)
        halo[1] = jnp.dot(beside_ref[1], stencil_ref[2], preferred_element_type=F32)

    stencils = jnp.concatenate([stencil_ref[0], stencil_ref[1], stencil_ref[2]], axis=1)
    for first in range(0, chunk, 2):
        tables = [jnp.concatenate([lifted_ref[first + slot], wide_ref[first + slot]], axis=0) for slot in range(2)]
        both = jnp.dot(spread[...], jnp.concatenate(tables, axis=1), preferred_element_type=F32)
        for slot in range(2):
            vector = pl.ds(step * chunk + first + slot, 1)
            three = jnp.dot(fine_ref[first + slot], stencils, preferred_element_type=F32)
            before[slot, pl.ds(7, 1), :] = halo[0, vector, :]
            before[slot, pl.ds(8, blocks), :] = three[:, :width]
            after[slot, pl.ds(0, blocks), :] = three[:, 2 * width :]
            after[slot, pl.ds(blocks, 1), :] = halo[1, vector, :]
            result = both[:, slot * width : (slot + 1) * width] + three[:, width : 2 * width]
            result = result + before[slot, pl.ds(7, blocks), :]
            out_ref[first + slot] = result + after[slot, pl.ds(1, blocks), :]


def whole(ndim_shape):
    return pl.BlockSpec(ndim_shape, lambda *_: (0,) * len(ndim_shape))


def shards(fine, pattern, stencil, restrict, coarse_inv):
    devices = lax.axis_size("gx")
    vectors, blocks, width = fine.shape
    levels, kinds = restrict.shape[:2]
    plan = Plan(devices, vectors, blocks, width, levels, kinds)
    stacked = restrict.reshape(levels, kinds * width, width)
    wide_count = len(plan.wide)
    params = pltpu.CompilerParams(dimension_semantics=("arbitrary",), vmem_limit_bytes=VMEM_LIMIT)
    chunk = 16
    steps = vectors // chunk
    near = plan.groups[plan.crossing[0]]
    far = devices // near
    crossing = len(plan.crossing)
    part = vectors // near
    vmem = pl.BlockSpec(memory_space=pltpu.VMEM)
    hbm = pl.BlockSpec(memory_space=pl.ANY)
    dma = pltpu.SemaphoreType.DMA
    lifted, wide, beside = pl.pallas_call(
        functools.partial(exchange_kernel, plan, chunk),
        out_shape=(
            jax.ShapeDtypeStruct((vectors, plan.narrow_rows, width), BF16),
            jax.ShapeDtypeStruct((vectors, plan.wide_rows, width), BF16),
            jax.ShapeDtypeStruct((2, vectors, width), BF16),
        ),
        in_specs=[vmem, hbm, hbm, hbm],
        out_specs=(hbm, hbm, vmem),
        scratch_shapes=[
            pltpu.VMEM(fine.shape, BF16),
            pltpu.VMEM(stacked.shape, BF16),
            pltpu.VMEM(coarse_inv.shape, BF16),
            pltpu.VMEM((vectors, plan.narrow_rows, width), BF16),
            pltpu.VMEM((vectors, plan.wide_rows, width), BF16),
            pltpu.VMEM((vectors, plan.wide_rows, width), F32),
            pltpu.VMEM((plan.wide_rows, blocks), BF16),
            pltpu.VMEM((plan.narrow_rows, blocks), BF16),
            pltpu.VMEM((chunk, plan.wide_rows, width), F32),
            pltpu.VMEM((chunk, plan.narrow_rows, width), BF16),
            pltpu.VMEM((plan.wide_used, vectors, width), BF16),
            pltpu.VMEM((wide_count, vectors, width), BF16),
            pltpu.VMEM((2, vectors, width), BF16),
            pltpu.VMEM((near, crossing, part, width), BF16),
            pltpu.VMEM((crossing, part, width), BF16),
            pltpu.VMEM((far, crossing - 1, part, width), BF16),
            pltpu.VMEM((crossing, part, width), BF16),
            pltpu.VMEM((near, crossing, part, width), BF16),
            dma((steps,)), dma((2,)), dma((steps,)), dma,
            dma((near,)), dma((near,)), dma((far,)), dma((far,)), dma((near,)), dma((near,)), dma((2,)), dma((2,)),
        ],
        compiler_params=pltpu.CompilerParams(
            collective_id=0, has_side_effects=True, vmem_limit_bytes=VMEM_LIMIT),
        name="exchange",
    )(pattern, fine, stacked, coarse_inv)

    last = 8
    return pl.pallas_call(
        functools.partial(final_kernel, plan, last),
        grid=(vectors // last,),
        out_shape=jax.ShapeDtypeStruct(fine.shape, F32),
        in_specs=[
            whole(pattern.shape), whole(beside.shape), whole(stencil.shape),
            pl.BlockSpec((last, blocks, width), lambda i: (i, 0, 0)),
            pl.BlockSpec((last, plan.narrow_rows, width), lambda i: (i, 0, 0)),
            pl.BlockSpec((last, plan.wide_rows, width), lambda i: (i, 0, 0)),
        ],
        out_specs=pl.BlockSpec((last, blocks, width), lambda i: (i, 0, 0)),
        scratch_shapes=[
            pltpu.VMEM((blocks, plan.narrow_rows + plan.wide_rows), BF16),
            pltpu.VMEM((2, vectors, width), F32),
            pltpu.VMEM((2, blocks + 8, width), F32),
            pltpu.VMEM((2, blocks + 8, width), F32),
        ],
        compiler_params=params,
        name="final",
    )(pattern, beside, stencil, fine, lifted, wide)


def solution(mesh):
    in_specs = (P(None, "gx", None), P(None, "gx"), P(), P(), P())
    out_specs = P(None, "gx", None)
    return jax.shard_map(shards, mesh=mesh, in_specs=in_specs, out_specs=out_specs, check_vma=False)
```
